256 devices in a mesh: mp: 64 (over y, z, core), dp: 4 (over x).
Axes of the slice: x: 4, y: 4, z: 8, core: 2. Of those that a mesh axis runs over, the one named last changes fastest.
Arguments:
- features: bfloat16 [256, 4, 4, 512], P(('dp', 'mp')), may hold values from 0 to 2
- labels: int32 [256], P('dp'), may hold values from 0 to 9
- subset_ids: int32 [64], P('mp'), may hold values from 0 to 255
- conv1_weight: bfloat16 [64, 9, 512, 512], P('mp'), may hold values from -0.09375 to 0.09375
- conv2_weight: bfloat16 [64, 9, 512, 512], P('mp'), may hold values from -0.09375 to 0.09375
- head_weight: float32 [64, 512, 10], P('mp'), may hold values from -0.25 to 0.25
Outputs:
- datamodel: float32 [256, 256], P(('dp', 'mp'))
- margin_mean: float32 [256], P(('dp', 'mp'))
- margin_norm: float32 [256], P(('dp', 'mp'))
The draws below stay inside these ranges and needn't reach their ends.
All inputs are finite; a program needn't handle non-finite values.
Results may differ from the reference program's by a relative error of at most 0.00077.
Values may be sent and summed in bfloat16 or wider, within the bound.
No kernel may reach another device: no remote copies, remote signals or barrier semaphores. Data moves between devices by JAX's collectives and lax.ppermute only.
A program may use at most 128 MiB of HBM per device.

```python
import jax
import jax.numpy as jnp
from jax import lax

C = 512
CLASSES = 10
SIDE = 4
SUBSETS = 256
TARGETS = 256
MODELS = 64


def with_ends(entries, own_key, low, high):
    dims = entries.shape
    spot = [jax.random.randint(jax.random.fold_in(own_key, axis), (), 0, dims[axis]) for axis in range(len(dims))]
    entries = entries.at[tuple(spot)].set(low)
    longest = dims.index(max(dims))
    spot[longest] = (spot[longest] + 1) % dims[longest]
    return entries.at[tuple(spot)].set(high)


def block_levels(key, shape, cuts, smallest, top_value):
    level = 1.0
    for dim, shards_of in cuts:
        draws = jax.random.uniform(jax.random.fold_in(jax.random.fold_in(key, 6), dim), (shards_of,), jnp.float32, smallest / len(cuts), top_value / len(cuts))
        level = level * jnp.repeat(jnp.exp(draws), shape[dim] // shards_of).reshape((-1,) + (1,) * (len(shape) - 1 - dim))
    return level


def bell_draw(stream_key, shape, deviation, reach, pieces=(), kind=jnp.bfloat16):
    drawn = deviation * jax.random.normal(stream_key, shape, jnp.float32)
    if pieces:
        drawn = drawn * block_levels(stream_key, shape, pieces, -0.22, 0.18)
    return jnp.clip(drawn, -reach, reach).astype(kind)


def setup_inputs(seed: int = 0) -> dict:
    streams_of = jax.random.split(jax.random.key(seed), 7)
    features = jnp.clip(2.0 * jax.random.uniform(streams_of[0], (TARGETS, SIDE, SIDE, C), jnp.float32) ** block_levels(streams_of[0], (TARGETS, SIDE, SIDE, C), ((0, 256),), -0.2, 0.2), 0.0, 2.0).astype(jnp.bfloat16)
    labels = with_ends(jax.random.randint(streams_of[1], (TARGETS,), 0, CLASSES), jax.random.fold_in(streams_of[1], 1), 0, CLASSES - 1).astype(jnp.int32)
    subset_ids = with_ends(jax.random.randint(streams_of[2], (MODELS,), 0, SUBSETS), jax.random.fold_in(streams_of[2], 1), 0, SUBSETS - 1).astype(jnp.int32)
    conv1_weight = bell_draw(streams_of[3], (MODELS, 9, C, C), (9 * C) ** -0.5, 0.09375, ((0, 64),))
    conv2_weight = bell_draw(streams_of[4], (MODELS, 9, C, C), (9 * C) ** -0.5, 0.09375, ((0, 64),))
    head_weight = bell_draw(streams_of[5], (MODELS, C, CLASSES), C ** -0.5, 0.25, ((0, 64),), jnp.float32)
    return {"features": features, "labels": labels, "subset_ids": subset_ids, "conv1_weight": conv1_weight, "conv2_weight": conv2_weight, "head_weight": head_weight}


def convolve(grid, kernel):
    batch = grid.shape[0]
    width = grid.shape[1]
    chans = grid.shape[3]
    padded = jnp.pad(grid, ((0, 0), (1, 1), (1, 1), (0, 0)))
    result = jnp.zeros((batch * width * width, kernel.shape[2]), jnp.float32)
    for offset in range(9):
        row_off, col_off = divmod(offset, 3)
        shifted = padded[:, row_off:row_off + width, col_off:col_off + width, :].reshape(batch * width * width, chans)
        result = result + jnp.dot(shifted, kernel[offset], preferred_element_type=jnp.float32)
    return result

def margins_of(grid, first_kernel, second_kernel, head, target_labels):
    batch = grid.shape[0]
    width = grid.shape[1]
    chans = grid.shape[3]
    hidden = jax.nn.relu(convolve(grid, first_kernel)).astype(jnp.bfloat16).reshape(batch, width, width, chans)
    branch = jax.nn.relu(convolve(hidden, second_kernel))
    blocked = grid.astype(jnp.float32).reshape(batch * width * width, chans) + branch
    pooled = lax.optimization_barrier(jnp.max(blocked.reshape(batch, width * width, chans), axis=1))
    logits = jnp.dot(pooled, head, precision=lax.Precision.HIGHEST, preferred_element_type=jnp.float32)
    classes = jnp.arange(head.shape[1], dtype=jnp.int32)[None, :]
    chosen = classes == target_labels[:, None]
    correct = lax.optimization_barrier(jnp.sum(jnp.where(chosen, logits, 0.0), axis=1))
    rival = lax.optimization_barrier(jnp.max(jnp.where(chosen, -1e+30, logits), axis=1))
    return correct - rival

def reference(features, labels, subset_ids, conv1_weight, conv2_weight, head_weight):

    def single(weights):
        return margins_of(features, weights[0], weights[1], weights[2], labels)
    margin = lax.map(single, (conv1_weight, conv2_weight, head_weight))
    model_count = margin.shape[0]
    margin_mean = lax.optimization_barrier(jnp.sum(margin, axis=0)) / model_count
    centred = margin - margin_mean[None, :]
    margin_norm = jnp.sqrt(1.0 + lax.optimization_barrier(jnp.sum(centred * centred, axis=0)) / model_count)
    scaled = centred / margin_norm[None, :]
    onehot = (subset_ids[:, None] == jnp.arange(SUBSETS, dtype=jnp.int32)[None, :]).astype(jnp.float32)
    datamodel = jnp.dot(scaled.T, onehot, precision=lax.Precision.HIGHEST, preferred_element_type=jnp.float32)
    return (datamodel, margin_mean, margin_norm)
```

```python
import functools

import jax
import jax.numpy as jnp
from jax import lax
from jax.experimental import pallas as pl
from jax.experimental.pallas import tpu as pltpu
from jax.sharding import Mesh, PartitionSpec as P

SIDE = 4
SPOTS = SIDE * SIDE
HALF = 256
CLASSES = 10
SUBSETS = 256
GROUP = 16

OFFSETS = (0, 1, 2, 3, 5, 6, 7, 8, 4)


def pairs_of(offset):
    row_off, col_off = offset // 3 - 1, offset % 3 - 1
    return [
        (r * SIDE + c, (r + row_off) * SIDE + c + col_off)
        for r in range(SIDE)
        for c in range(SIDE)
        if 0 <= r + row_off < SIDE and 0 <= c + col_off < SIDE
    ]


def convolve(source, weight, accs):
    stage = 0
    for offset in OFFSETS:
        pairs = pairs_of(offset)
        for k in range(2):
            deep = pl.ds(k * HALF, HALF)
            for n in range(2):
                pltpu.matmul_push_rhs(
                    weight[offset, deep, pl.ds(n * HALF, HALF)], staging_register=stage, mxu_index=n
                )
            for i, (spot, origin) in enumerate(pairs):
                rows = source[origin, :, deep]
                for n in range(2):
                    pltpu.matmul_acc_lhs(
                        accs[n][spot], rows, load_staged_rhs=stage if i == 0 else None
                    )
            stage = 1 - stage


def by_position(sources, moved, accs):
    lane = lax.broadcasted_iota(jnp.int32, (GROUP, HALF), 1)
    target = lax.broadcasted_iota(jnp.int32, (GROUP, HALF), 0)
    picks = [
        jnp.where(lane == target * SPOTS + spot, 1.0, 0.0).astype(jnp.bfloat16)
        for spot in range(SPOTS)
    ]
    pick = jnp.concatenate(picks, axis=0)
    for g, (ref, start) in enumerate(sources):
        for n in range(2):
            pltpu.matmul_push_rhs(
                ref[pl.ds(start, HALF), pl.ds(n * HALF, HALF)], staging_register=g % 2, mxu_index=n
            )
            pltpu.matmul_acc_lhs(accs[n][g], pick, load_staged_rhs=g % 2)
    for g in range(len(sources)):
        for n in range(2):
            got = pltpu.matmul_pop(accs[n][g]).astype(jnp.bfloat16)
            moved[:, pl.ds(g * GROUP, GROUP), pl.ds(n * HALF, HALF)] = got.reshape(SPOTS, GROUP, HALF)


def conv_kernel(core, ident, own, other, w1, w2, head, labels, out, moved, hidden, pooled):
    targets = moved.shape[1]
    groups = targets // GROUP
    sources = [(own, i * HALF) for i in range(groups // 2)] + [(other, i * HALF) for i in range(groups // 2)]

    def shuffle(*flat):
        by_position(sources, moved, (flat[:groups], flat[groups:]))

    pl.run_scoped(
        shuffle,
        *[pltpu.ACC(n)((HALF, HALF), jnp.float32) for n in range(2) for _ in range(groups)],
    )

    def both(*flat):
        accs = (flat[:SPOTS], flat[SPOTS:])
        convolve(moved, w1, accs)
        for spot in range(SPOTS):
            for n in range(2):
                got = jnp.maximum(pltpu.matmul_pop(accs[n][spot]), 0.0)
                hidden[spot, :, pl.ds(n * HALF, HALF)] = got.astype(jnp.bfloat16)
        convolve(hidden, w2, accs)
        for spot in range(SPOTS):
            for n in range(2):
                cols = pl.ds(n * HALF, HALF)
                got = jnp.maximum(pltpu.matmul_pop(accs[n][spot]), 0.0)
                got = got + moved[spot, :, cols].astype(jnp.float32)
                if spot:
                    got = jnp.maximum(got, pooled[:, cols])
                pooled[:, cols] = got

    pl.run_scoped(
        both,
        *[pltpu.ACC(n)((targets, HALF), jnp.float32) for n in range(2) for _ in range(SPOTS)],
    )

    wide = (targets, 128)
    lane = lax.broadcasted_iota(jnp.int32, wide, 1)
    logits = jnp.full(wide, -1e30, jnp.float32)
    for k in range(CLASSES):
        total = pooled[:, pl.ds(0, 128)] * head[pl.ds(k, 1), pl.ds(0, 128)]
        for j in range(1, 4):
            cols = pl.ds(j * 128, 128)
            total = total + pooled[:, cols] * head[pl.ds(k, 1), cols]
        logits = jnp.where(lane == k, jnp.sum(total, axis=1, keepdims=True), logits)
    chosen = lane == labels[...]
    correct = jnp.sum(jnp.where(chosen, logits, 0.0), axis=1, keepdims=True)
    rival = jnp.max(jnp.where(chosen, -1e30, logits), axis=1, keepdims=True)
    ident_f = ident[0].astype(jnp.float32)
    packed = jnp.where(lane < 64, correct - rival, ident_f)
    half = targets // 2
    for j in range(half):
        out[pl.ds(2 * j + core[0], 1), 0, :] = packed[j : j + 1, :]
        out[pl.ds(2 * j + 1 - core[0], 1), 0, :] = packed[half + j : half + j + 1, :]


def conv_call(core, ident, own, other, w1, w2, head, labels):
    targets = 2 * own.shape[0] // SPOTS
    smem = pl.BlockSpec(memory_space=pltpu.SMEM)
    vmem = pl.BlockSpec(memory_space=pltpu.VMEM)
    return pl.pallas_call(
        conv_kernel,
        out_shape=jax.ShapeDtypeStruct((targets, 1, 128), jnp.float32),
        in_specs=[smem, smem] + [vmem] * 6,
        out_specs=vmem,
        scratch_shapes=[
            pltpu.VMEM((SPOTS, targets, 512), jnp.bfloat16),
            pltpu.VMEM((SPOTS, targets, 512), jnp.bfloat16),
            pltpu.VMEM((targets, 512), jnp.float32),
        ],
        compiler_params=pltpu.CompilerParams(vmem_limit_bytes=40 * 1024 * 1024),
        name="margins",
    )(core, ident, own, other, w1, w2, head, labels)


def tail_kernel(columns, datamodel, mean_out, norm_out):
    models = columns.shape[0]
    rows = columns[:, 0, :]
    lane = lax.broadcasted_iota(jnp.int32, rows.shape, 1)
    margin = jnp.max(jnp.where(lane < 64, rows, -3e38), axis=1, keepdims=True)
    ident = jnp.max(jnp.where(lane < 64, -1.0, rows), axis=1, keepdims=True)
    mean = jnp.sum(margin, axis=0, keepdims=True) / models
    centred = margin - mean
    norm = jnp.sqrt(1.0 + jnp.sum(centred * centred, axis=0, keepdims=True) / models)
    scaled = centred / norm
    subset = lax.broadcasted_iota(jnp.int32, (models, SUBSETS), 1).astype(jnp.float32)
    datamodel[...] = jnp.sum(jnp.where(subset == ident, scaled, 0.0), axis=0, keepdims=True)
    mean_out[...] = jnp.broadcast_to(mean, mean_out.shape)
    norm_out[...] = jnp.broadcast_to(norm, norm_out.shape)


def tail_call(columns):
    vmem = pl.BlockSpec(memory_space=pltpu.VMEM)
    return pl.pallas_call(
        tail_kernel,
        out_shape=(
            jax.ShapeDtypeStruct((1, SUBSETS), jnp.float32),
            jax.ShapeDtypeStruct((1, 128), jnp.float32),
            jax.ShapeDtypeStruct((1, 128), jnp.float32),
        ),
        in_specs=[vmem],
        out_specs=(vmem, vmem, vmem),
        name="statistics",
    )(columns)


def exchanged(x, axis):
    return lax.all_to_all(x, axis, 0, 0, tiled=True)


def shards(features, labels, subset_ids, conv1_weight, conv2_weight, head_weight):
    across_z, across_y = lax.axis_size("z"), lax.axis_size("y")
    core = lax.axis_index("core").astype(jnp.int32)
    grid = features.reshape(1, SPOTS, 512)
    column = exchanged(jnp.broadcast_to(grid, (across_z, SPOTS, 512)), "z")
    plane = exchanged(jnp.broadcast_to(column[None], (across_y, *column.shape)), "y")
    own = plane.reshape(-1, 512)
    other = lax.ppermute(own, "core", ((0, 1), (1, 0)))
    pairs = labels.reshape(-1, 2)
    order = jnp.where(core == 0, pairs.T, pairs[:, ::-1].T).reshape(-1, 1)
    wide_labels = jnp.broadcast_to(order, (order.shape[0], 128))
    packed = conv_call(
        core.reshape(1),
        subset_ids,
        own,
        other,
        conv1_weight[0],
        conv2_weight[0],
        head_weight[0].T,
        wide_labels,
    )
    columns = exchanged(packed, ("y", "z", "core"))
    datamodel, mean, norm = tail_call(columns)
    return (datamodel, mean[0, :1], norm[0, :1])


def solution(mesh):
    fine = Mesh(mesh.devices.reshape(4, 8, 2, 4), ("y", "z", "core", "dp"))
    mp = ("y", "z", "core")
    every = ("dp", *mp)
    in_specs = (
        P(every, None, None, None),
        P("dp"),
        P(mp),
        P(mp, None, None, None),
        P(mp, None, None, None),
        P(mp, None, None),
    )
    out_specs = (P(every, None), P(every), P(every))
    return jax.shard_map(shards, mesh=fine, in_specs=in_specs, out_specs=out_specs, check_vma=False)
```

```python
import functools

import jax
import jax.numpy as jnp
from jax import lax
from jax.experimental import pallas as pl
from jax.experimental.pallas import tpu as pltpu
from jax.sharding import Mesh, PartitionSpec as P

SIDE = 4
SPOTS = SIDE * SIDE
HALF = 256
CLASSES = 10
SUBSETS = 256
GROUP = 16

OFFSETS = (0, 1, 2, 3, 5, 6, 7, 8, 4)


def pairs_of(offset):
    row_off, col_off = offset // 3 - 1, offset % 3 - 1
    return [
        (r * SIDE + c, (r + row_off) * SIDE + c + col_off)
        for r in range(SIDE)
        for c in range(SIDE)
        if 0 <= r + row_off < SIDE and 0 <= c + col_off < SIDE
    ]


def convolve(source, weight, accs, arrive=None):
    stage = 0
    for offset in OFFSETS:
        pairs = pairs_of(offset)
        if arrive is not None:
            arrive(offset)
        for k in range(2):
            deep = pl.ds(k * HALF, HALF)
            for n in range(2):
                pltpu.matmul_push_rhs(
                    weight[offset, deep, pl.ds(n * HALF, HALF)], staging_register=stage, mxu_index=n
                )
            for i, (spot, origin) in enumerate(pairs):
                rows = source[origin, :, deep]
                for n in range(2):
                    pltpu.matmul_acc_lhs(
                        accs[n][spot], rows, load_staged_rhs=stage if i == 0 else None
                    )
            stage = 1 - stage


def by_position(sources, moved, accs):
    lane = lax.broadcasted_iota(jnp.int32, (GROUP, HALF), 1)
    target = lax.broadcasted_iota(jnp.int32, (GROUP, HALF), 0)
    picks = [
        jnp.where(lane == target * SPOTS + spot, 1.0, 0.0).astype(jnp.bfloat16)
        for spot in range(SPOTS)
    ]
    pick = jnp.concatenate(picks, axis=0)
    for g, refs in enumerate(sources):
        for n in range(2):
            block = [ref[:, :, pl.ds(n * HALF, HALF)].reshape(-1, HALF) for ref in refs]
            pltpu.matmul_push_rhs(
                jnp.concatenate(block, axis=0), staging_register=g % 2, mxu_index=n
            )
            pltpu.matmul_acc_lhs(accs[n][g], pick, load_staged_rhs=g % 2)
    for g in range(len(sources)):
        for n in range(2):
            got = pltpu.matmul_pop(accs[n][g]).astype(jnp.bfloat16)
            moved[:, pl.ds(g * GROUP, GROUP), pl.ds(n * HALF, HALF)] = got.reshape(SPOTS, GROUP, HALF)


class Stream:
    AHEAD = 6

    def __init__(self, pairs, sems):
        self.copies = [
            pltpu.make_async_copy(src.at[offset], dst.at[offset], sems.at[i, offset])
            for i, (src, dst) in enumerate(pairs)
            for offset in OFFSETS
        ]
        self.started = self.waited = 0
        for _ in range(self.AHEAD):
            self.start()

    def start(self):
        if self.started < len(self.copies):
            self.copies[self.started].start()
            self.started += 1

    def arrive(self, offset):
        self.copies[self.waited].wait()
        self.waited += 1
        self.start()


def conv_kernel(columns, fetch, *refs):
    ident, labels, head, w1, w2 = refs[:5]
    grids = refs[5 : 5 + len(columns)]
    if fetch:
        out, o1, o2, moved, hidden, pooled, sems = refs[-7:]
        arrive = Stream(((w1, o1), (w2, o2)), sems).arrive
        w1, w2 = o1, o2
    else:
        out, moved, hidden, pooled = refs[-4:]
        arrive = None
    targets = moved.shape[1]
    deep = grids[0].shape[0]
    groups = targets // GROUP
    sources = [grids[2 * g : 2 * g + 2] for g in range(groups)]

    def shuffle(*flat):
        by_position(sources, moved, (flat[:groups], flat[groups:]))

    pl.run_scoped(
        shuffle,
        *[pltpu.ACC(n)((HALF, HALF), jnp.float32) for n in range(2) for _ in range(groups)],
    )

    def both(*flat):
        accs = (flat[:SPOTS], flat[SPOTS:])
        convolve(moved, w1, accs, arrive)
        for spot in range(SPOTS):
            for n in range(2):
                got = jnp.maximum(pltpu.matmul_pop(accs[n][spot]), 0.0)
                hidden[spot, :, pl.ds(n * HALF, HALF)] = got.astype(jnp.bfloat16)
        convolve(hidden, w2, accs, arrive)
        for spot in range(SPOTS):
            for n in range(2):
                cols = pl.ds(n * HALF, HALF)
                got = jnp.maximum(pltpu.matmul_pop(accs[n][spot]), 0.0)
                got = got + moved[spot, :, cols].astype(jnp.float32)
                if spot:
                    got = jnp.maximum(got, pooled[:, cols])
                pooled[:, cols] = got

    pl.run_scoped(
        both,
        *[pltpu.ACC(n)((targets, HALF), jnp.float32) for n in range(2) for _ in range(SPOTS)],
    )

    core, y = lax.axis_index("core"), lax.axis_index("y")
    rows = []
    for steps, swap in columns:
        first = lax.rem(y + steps, lax.axis_size("y")) * (2 * deep)
        first = first + (1 - core if swap else core)
        rows += [first + 2 * z for z in range(deep)]
    wide = (targets, 128)
    lane = lax.broadcasted_iota(jnp.int32, wide, 1)
    line = lax.broadcasted_iota(jnp.int32, wide, 0)
    label = jnp.zeros(wide, jnp.int32)
    for i, row in enumerate(rows):
        label = jnp.where(line == i, labels[row], label)
    logits = jnp.full(wide, -1e30, jnp.float32)
    for k in range(CLASSES):
        total = pooled[:, pl.ds(0, 128)] * head[k, :, pl.ds(0, 128)]
        for j in range(1, 4):
            cols = pl.ds(j * 128, 128)
            total = total + pooled[:, cols] * head[k, :, cols]
        logits = jnp.where(lane == k, jnp.sum(total, axis=1, keepdims=True), logits)
    chosen = lane == label
    correct = jnp.sum(jnp.where(chosen, logits, 0.0), axis=1, keepdims=True)
    rival = jnp.max(jnp.where(chosen, -1e30, logits), axis=1, keepdims=True)
    packed = jnp.where(lane < 64, correct - rival, ident[0].astype(jnp.float32))
    for i, row in enumerate(rows):
        out[pl.ds(row, 1), 0, :] = packed[i : i + 1, :]


def in_vmem(x):
    return pltpu.with_memory_space_constraint(x, pltpu.VMEM)


def in_hbm(x):
    return pltpu.with_memory_space_constraint(x, pltpu.HBM)


def conv_call(columns, grids, ident, labels, head, w1, w2, before=None):
    fetch = before is None
    targets = sum(grid.shape[0] for grid in grids)
    smem = pl.BlockSpec(memory_space=pltpu.SMEM)
    vmem = pl.BlockSpec(memory_space=pltpu.VMEM)
    hbm = pl.BlockSpec(memory_space=pltpu.HBM)
    result = pltpu.VMEM((64, 1, 128), jnp.float32)
    scratch = [
        pltpu.VMEM((SPOTS, targets, 512), jnp.bfloat16),
        pltpu.VMEM((SPOTS, targets, 512), jnp.bfloat16),
        pltpu.VMEM((targets, 512), jnp.float32),
    ]
    operands = [ident, labels, head]
    aliases = {}
    if fetch:
        operands += [in_hbm(w1), in_hbm(w2), *map(in_vmem, grids)]
        specs = [smem, smem, vmem, hbm, hbm] + [vmem] * len(grids)
        out_shape = (result, pltpu.VMEM(w1.shape, w1.dtype), pltpu.VMEM(w2.shape, w2.dtype))
        out_specs = (vmem, vmem, vmem)
        scratch.append(pltpu.SemaphoreType.DMA((2, w1.shape[0])))
    else:
        aliases = {len(operands) + 2 + len(grids): 0}
        operands += [in_vmem(w1), in_vmem(w2), *map(in_vmem, grids), in_vmem(before)]
        specs = [smem, smem] + [vmem] * (4 + len(grids))
        out_shape, out_specs = result, vmem
    work = 2 * 100 * targets * 512 * 512 * 2
    return pl.pallas_call(
        functools.partial(conv_kernel, columns, fetch),
        out_shape=out_shape,
        in_specs=specs,
        out_specs=out_specs,
        scratch_shapes=scratch,
        input_output_aliases=aliases,
        cost_estimate=pl.CostEstimate(flops=work, bytes_accessed=1 << 20, transcendentals=0),
        compiler_params=pltpu.CompilerParams(vmem_limit_bytes=16 * 1024 * 1024),
        name=f"margins_{columns[0][0]}_{int(columns[0][1])}",
    )(*operands)


def tail_kernel(columns, datamodel, mean_out, norm_out):
    models = columns.shape[0]
    rows = columns[:, 0, :]
    lane = lax.broadcasted_iota(jnp.int32, rows.shape, 1)
    margin = jnp.max(jnp.where(lane < 64, rows, -3e38), axis=1, keepdims=True)
    ident = jnp.max(jnp.where(lane < 64, -1.0, rows), axis=1, keepdims=True)
    mean = jnp.sum(margin, axis=0, keepdims=True) / models
    centred = margin - mean
    norm = jnp.sqrt(1.0 + jnp.sum(centred * centred, axis=0, keepdims=True) / models)
    scaled = centred / norm
    subset = lax.broadcasted_iota(jnp.int32, (models, SUBSETS), 1).astype(jnp.float32)
    datamodel[...] = jnp.sum(jnp.where(subset == ident, scaled, 0.0), axis=0, keepdims=True)
    mean_out[...] = jnp.broadcast_to(mean, mean_out.shape)
    norm_out[...] = jnp.broadcast_to(norm, norm_out.shape)


def tail_call(columns):
    vmem = pl.BlockSpec(memory_space=pltpu.VMEM)
    return pl.pallas_call(
        tail_kernel,
        out_shape=(
            jax.ShapeDtypeStruct((1, SUBSETS), jnp.float32),
            jax.ShapeDtypeStruct((1, 128), jnp.float32),
            jax.ShapeDtypeStruct((1, 128), jnp.float32),
        ),
        in_specs=[vmem],
        out_specs=(vmem, vmem, vmem),
        compiler_params=pltpu.CompilerParams(vmem_limit_bytes=1024 * 1024),
        name="statistics",
    )(columns)


def exchanged(x, axis):
    return lax.all_to_all(x, axis, 0, 0, tiled=True)


def shifted(x, axis, step):
    size = lax.axis_size(axis)
    return lax.ppermute(x, axis, [(i, (i + step) % size) for i in range(size)])


def shards(features, labels, subset_ids, conv1_weight, conv2_weight, head_weight):
    grid = features.reshape(1, SPOTS, 512)
    spread = jnp.broadcast_to(grid, (lax.axis_size("z"), SPOTS, 512))
    column = exchanged(spread, "z")
    head = jnp.transpose(head_weight, (2, 0, 1))
    fixed = (subset_ids, labels, head)
    column_o = shifted(column, "core", 1)
    three, one, two = (shifted(column, "y", step) for step in (1, -1, 2))
    packed, w1, w2 = conv_call(
        ((0, False), (0, True)), (column, column_o), *fixed, conv1_weight[0], conv2_weight[0]
    )
    fixed = (*fixed, w1, w2)
    three, one, packed = lax.optimization_barrier((three, one, packed))
    three_o, one_o = shifted(three, "core", 1), shifted(one, "core", 1)
    packed = conv_call(((3, False), (1, False)), (three, one), *fixed, packed)
    two, packed = lax.optimization_barrier((two, packed))
    two_o = shifted(two, "core", 1)
    packed = conv_call(((3, True), (1, True)), (three_o, one_o), *fixed, packed)
    packed = conv_call(((2, False), (2, True)), (two, two_o), *fixed, packed)
    columns = exchanged(packed, ("y", "z", "core"))
    datamodel, mean, norm = tail_call(columns)
    return (datamodel, mean[0, :1], norm[0, :1])


def solution(mesh):
    fine = Mesh(mesh.devices.reshape(4, 8, 2, 4), ("y", "z", "core", "dp"))
    mp = ("y", "z", "core")
    every = ("dp", *mp)
    in_specs = (
        P(every, None, None, None),
        P("dp"),
        P(mp),
        P(mp, None, None, None),
        P(mp, None, None, None),
        P(mp, None, None),
    )
    out_specs = (P(every, None), P(every), P(every))
    return jax.shard_map(shards, mesh=fine, in_specs=in_specs, out_specs=out_specs, check_vma=False)
```

```python
import functools

import jax
import jax.numpy as jnp
from jax import lax
from jax.experimental import pallas as pl
from jax.experimental.pallas import tpu as pltpu
from jax.sharding import Mesh, PartitionSpec as P

SIDE = 4
SPOTS = SIDE * SIDE
HALF = 256
CLASSES = 10
SUBSETS = 256
GROUP = 16

OFFSETS = (0, 1, 2, 3, 5, 6, 7, 8, 4)


def pairs_of(offset):
    row_off, col_off = offset // 3 - 1, offset % 3 - 1
    return [
        (r * SIDE + c, (r + row_off) * SIDE + c + col_off)
        for r in range(SIDE)
        for c in range(SIDE)
        if 0 <= r + row_off < SIDE and 0 <= c + col_off < SIDE
    ]


def convolve(source, weight, accs):
    stage = 0
    for offset in OFFSETS:
        pairs = pairs_of(offset)
        for k in range(2):
            deep = pl.ds(k * HALF, HALF)
            for n in range(2):
                pltpu.matmul_push_rhs(
                    weight[offset, deep, pl.ds(n * HALF, HALF)], staging_register=stage, mxu_index=n
                )
            for i, (spot, origin) in enumerate(pairs):
                rows = source[origin, :, deep]
                for n in range(2):
                    pltpu.matmul_acc_lhs(
                        accs[n][spot], rows, load_staged_rhs=stage if i == 0 else None
                    )
            stage = 1 - stage


def by_position(sources, moved, accs):
    lane = lax.broadcasted_iota(jnp.int32, (GROUP, HALF), 1)
    target = lax.broadcasted_iota(jnp.int32, (GROUP, HALF), 0)
    picks = [
        jnp.where(lane == target * SPOTS + spot, 1.0, 0.0).astype(jnp.bfloat16)
        for spot in range(SPOTS)
    ]
    pick = jnp.concatenate(picks, axis=0)
    for g, refs in enumerate(sources):
        for n in range(2):
            block = [ref[:, :, pl.ds(n * HALF, HALF)].reshape(-1, HALF) for ref in refs]
            pltpu.matmul_push_rhs(
                jnp.concatenate(block, axis=0), staging_register=g % 2, mxu_index=n
            )
            pltpu.matmul_acc_lhs(accs[n][g], pick, load_staged_rhs=g % 2)
    for g in range(len(sources)):
        for n in range(2):
            got = pltpu.matmul_pop(accs[n][g]).astype(jnp.bfloat16)
            moved[:, pl.ds(g * GROUP, GROUP), pl.ds(n * HALF, HALF)] = got.reshape(SPOTS, GROUP, HALF)


def conv_kernel(columns, *refs):
    ident, labels, head, w1, w2 = refs[:5]
    grids = refs[5 : 5 + len(columns)]
    out, moved, hidden, pooled = refs[-4:]
    targets = moved.shape[1]
    deep = grids[0].shape[0]
    groups = targets // GROUP
    sources = [grids[2 * g : 2 * g + 2] for g in range(groups)]

    def shuffle(*flat):
        by_position(sources, moved, (flat[:groups], flat[groups:]))

    pl.run_scoped(
        shuffle,
        *[pltpu.ACC(n)((HALF, HALF), jnp.float32) for n in range(2) for _ in range(groups)],
    )

    def both(*flat):
        accs = (flat[:SPOTS], flat[SPOTS:])
        convolve(moved, w1, accs)
        for spot in range(SPOTS):
            for n in range(2):
                got = jnp.maximum(pltpu.matmul_pop(accs[n][spot]), 0.0)
                hidden[spot, :, pl.ds(n * HALF, HALF)] = got.astype(jnp.bfloat16)
        convolve(hidden, w2, accs)
        for spot in range(SPOTS):
            for n in range(2):
                cols = pl.ds(n * HALF, HALF)
                got = jnp.maximum(pltpu.matmul_pop(accs[n][spot]), 0.0)
                got = got + moved[spot, :, cols].astype(jnp.float32)
                if spot:
                    got = jnp.maximum(got, pooled[:, cols])
                pooled[:, cols] = got

    pl.run_scoped(
        both,
        *[pltpu.ACC(n)((targets, HALF), jnp.float32) for n in range(2) for _ in range(SPOTS)],
    )

    core, y = lax.axis_index("core"), lax.axis_index("y")
    firsts = []
    for steps, swap in columns:
        first = lax.rem(y + steps, lax.axis_size("y")) * (2 * deep)
        firsts.append(first + (1 - core if swap else core))
    wide = (targets, 128)
    lane = lax.broadcasted_iota(jnp.int32, wide, 1)
    line = lax.broadcasted_iota(jnp.int32, wide, 0)
    place = 2 * (line & (deep - 1))
    for i, first in enumerate(firsts):
        place = place + jnp.where(line // deep == i, first, 0)
    few = labels.shape[1]
    spread_labels = jnp.broadcast_to(labels[...].astype(jnp.float32), (targets, few))
    mine = jnp.where(place[:, :few] == lane[:, :few], spread_labels, 0.0)
    label = jnp.sum(mine, axis=1, keepdims=True).astype(jnp.int32)
    logits = jnp.full(wide, -1e30, jnp.float32)
    for k in range(CLASSES):
        total = pooled[:, pl.ds(0, 128)] * head[k, :, pl.ds(0, 128)]
        for j in range(1, 4):
            cols = pl.ds(j * 128, 128)
            total = total + pooled[:, cols] * head[k, :, cols]
        logits = jnp.where(lane == k, jnp.sum(total, axis=1, keepdims=True), logits)
    chosen = lane == label
    correct = jnp.sum(jnp.where(chosen, logits, 0.0), axis=1, keepdims=True)
    rival = jnp.max(jnp.where(chosen, -1e30, logits), axis=1, keepdims=True)
    packed = jnp.where(lane < 64, correct - rival, ident[0].astype(jnp.float32))
    for i in range(targets):
        out[pl.ds(firsts[i // deep] + 2 * (i % deep), 1), 0, :] = packed[i : i + 1, :]


def in_vmem(x):
    return pltpu.with_memory_space_constraint(x, pltpu.VMEM)


def conv_call(columns, grids, ident, labels, head, w1, w2, before=None):
    targets = sum(grid.shape[0] for grid in grids)
    operands = [ident, labels, head, *map(in_vmem, (w1, w2, *grids))]
    aliases = {}
    if before is not None:
        aliases = {len(operands): 0}
        operands.append(in_vmem(before))
    vmem = pl.BlockSpec(memory_space=pltpu.VMEM)
    work = 2 * 100 * targets * 512 * 512 * 2
    return pl.pallas_call(
        functools.partial(conv_kernel, columns),
        out_shape=pltpu.VMEM((64, 1, 128), jnp.float32),
        in_specs=[pl.BlockSpec(memory_space=pltpu.SMEM)] + [vmem] * (len(operands) - 1),
        out_specs=vmem,
        scratch_shapes=[
            pltpu.VMEM((SPOTS, targets, 512), jnp.bfloat16),
            pltpu.VMEM((SPOTS, targets, 512), jnp.bfloat16),
            pltpu.VMEM((targets, 512), jnp.float32),
        ],
        input_output_aliases=aliases,
        cost_estimate=pl.CostEstimate(flops=work, bytes_accessed=1 << 20, transcendentals=0),
        compiler_params=pltpu.CompilerParams(vmem_limit_bytes=16 * 1024 * 1024),
        name=f"margins_{columns[0][0]}_{int(columns[0][1])}",
    )(*operands)


def spread_kernel(grid, out):
    flat = grid[...].reshape(SPOTS, grid.shape[-1])
    for i in range(out.shape[0]):
        out[i] = flat


def spread_call(grid, copies):
    return pl.pallas_call(
        spread_kernel,
        out_shape=pltpu.VMEM((copies, SPOTS, grid.shape[-1]), grid.dtype),
        in_specs=[pl.BlockSpec(memory_space=pltpu.VMEM)],
        out_specs=pl.BlockSpec(memory_space=pltpu.VMEM),
        cost_estimate=pl.CostEstimate(flops=10**10, bytes_accessed=1 << 25, transcendentals=0),
        compiler_params=pltpu.CompilerParams(vmem_limit_bytes=1024 * 1024),
        name="spread",
    )(grid)


def tail_kernel(columns, datamodel, mean_out, norm_out):
    models = columns.shape[0]
    rows = columns[:, 0, :]
    lane = lax.broadcasted_iota(jnp.int32, rows.shape, 1)
    margin = jnp.max(jnp.where(lane < 64, rows, -3e38), axis=1, keepdims=True)
    ident = jnp.max(jnp.where(lane < 64, -1.0, rows), axis=1, keepdims=True)
    mean = jnp.sum(margin, axis=0, keepdims=True) / models
    centred = margin - mean
    norm = jnp.sqrt(1.0 + jnp.sum(centred * centred, axis=0, keepdims=True) / models)
    scaled = centred / norm
    subset = lax.broadcasted_iota(jnp.int32, (models, SUBSETS), 1).astype(jnp.float32)
    datamodel[...] = jnp.sum(jnp.where(subset == ident, scaled, 0.0), axis=0, keepdims=True)
    mean_out[...] = jnp.broadcast_to(mean, mean_out.shape)
    norm_out[...] = jnp.broadcast_to(norm, norm_out.shape)


def tail_call(columns):
    vmem = pl.BlockSpec(memory_space=pltpu.VMEM)
    return pl.pallas_call(
        tail_kernel,
        out_shape=(
            jax.ShapeDtypeStruct((1, SUBSETS), jnp.float32),
            jax.ShapeDtypeStruct((1, 128), jnp.float32),
            jax.ShapeDtypeStruct((1, 128), jnp.float32),
        ),
        in_specs=[vmem],
        out_specs=(vmem, vmem, vmem),
        compiler_params=pltpu.CompilerParams(vmem_limit_bytes=1024 * 1024),
        name="statistics",
    )(columns)


def exchanged(x, axis):
    return lax.all_to_all(x, axis, 0, 0, tiled=True)


def shifted(x, axis, step):
    size = lax.axis_size(axis)
    return lax.ppermute(x, axis, [(i, (i + step) % size) for i in range(size)])


def shards(features, labels, subset_ids, conv1_weight, conv2_weight, head_weight):
    column = exchanged(spread_call(features[0], lax.axis_size("z")), "z")
    head = jnp.transpose(head_weight, (2, 0, 1))
    fixed = (subset_ids, labels.reshape(1, -1), head, conv1_weight[0], conv2_weight[0])
    column_o = shifted(column, "core", 1)
    three, one, two = (shifted(column, "y", step) for step in (1, -1, 2))
    packed = conv_call(((0, False), (0, True)), (column, column_o), *fixed)
    three, one, two, packed = lax.optimization_barrier((three, one, two, packed))
    three_o, one_o, two_o = (shifted(x, "core", 1) for x in (three, one, two))
    packed = conv_call(((3, False), (1, False)), (three, one), *fixed, packed)
    packed = conv_call(
        ((3, True), (1, True), (2, False), (2, True)), (three_o, one_o, two, two_o), *fixed, packed
    )
    columns = exchanged(packed, ("y", "z", "core"))
    datamodel, mean, norm = tail_call(columns)
    return (datamodel, mean[0, :1], norm[0, :1])


def solution(mesh):
    fine = Mesh(mesh.devices.reshape(4, 8, 2, 4), ("y", "z", "core", "dp"))
    mp = ("y", "z", "core")
    every = ("dp", *mp)
    in_specs = (
        P(every, None, None, None),
        P("dp"),
        P(mp),
        P(mp, None, None, None),
        P(mp, None, None, None),
        P(mp, None, None),
    )
    out_specs = (P(every, None), P(every), P(every))
    return jax.shard_map(shards, mesh=fine, in_specs=in_specs, out_specs=out_specs, check_vma=False)
```

```python
import functools

import jax
import jax.numpy as jnp
from jax import lax
from jax.experimental import pallas as pl
from jax.experimental.pallas import tpu as pltpu
from jax.sharding import Mesh, PartitionSpec as P

SIDE = 4
SPOTS = SIDE * SIDE
HALF = 256
CLASSES = 10
SUBSETS = 256
GROUP = 16

OFFSETS = (0, 1, 2, 3, 5, 6, 7, 8, 4)


def pairs_of(offset):
    row_off, col_off = offset // 3 - 1, offset % 3 - 1
    return [
        (r * SIDE + c, (r + row_off) * SIDE + c + col_off)
        for r in range(SIDE)
        for c in range(SIDE)
        if 0 <= r + row_off < SIDE and 0 <= c + col_off < SIDE
    ]


def convolve(source, weight, accs):
    stage = 0
    for offset in OFFSETS:
        pairs = pairs_of(offset)
        for k in range(2):
            deep = pl.ds(k * HALF, HALF)
            for n in range(2):
                pltpu.matmul_push_rhs(
                    weight[offset, deep, pl.ds(n * HALF, HALF)], staging_register=stage, mxu_index=n
                )
            for i, (spot, origin) in enumerate(pairs):
                rows = source[origin, :, deep]
                for n in range(2):
                    pltpu.matmul_acc_lhs(
                        accs[n][spot], rows, load_staged_rhs=stage if i == 0 else None
                    )
            stage = 1 - stage


def by_position(sources, moved, accs):
    lane = lax.broadcasted_iota(jnp.int32, (GROUP, HALF), 1)
    target = lax.broadcasted_iota(jnp.int32, (GROUP, HALF), 0)
    picks = [
        jnp.where(lane == target * SPOTS + spot, 1.0, 0.0).astype(jnp.bfloat16)
        for spot in range(SPOTS)
    ]
    pick = jnp.concatenate(picks, axis=0)
    for g, refs in enumerate(sources):
        for n in range(2):
            block = [ref[:, :, pl.ds(n * HALF, HALF)].reshape(-1, HALF) for ref in refs]
            pltpu.matmul_push_rhs(
                jnp.concatenate(block, axis=0), staging_register=g % 2, mxu_index=n
            )
            pltpu.matmul_acc_lhs(accs[n][g], pick, load_staged_rhs=g % 2)
    for g in range(len(sources)):
        for n in range(2):
            got = pltpu.matmul_pop(accs[n][g]).astype(jnp.bfloat16)
            moved[:, pl.ds(g * GROUP, GROUP), pl.ds(n * HALF, HALF)] = got.reshape(SPOTS, GROUP, HALF)


def conv_kernel(columns, *refs):
    ident, labels, head, w1, w2 = refs[:5]
    grids = refs[5 : 5 + len(columns)]
    out, moved, hidden, pooled = refs[-4:]
    targets = moved.shape[1]
    deep = grids[0].shape[0]
    groups = targets // GROUP
    sources = [grids[2 * g : 2 * g + 2] for g in range(groups)]

    def shuffle(*flat):
        by_position(sources, moved, (flat[:groups], flat[groups:]))

    pl.run_scoped(
        shuffle,
        *[pltpu.ACC(n)((HALF, HALF), jnp.float32) for n in range(2) for _ in range(groups)],
    )

    def both(*flat):
        accs = (flat[:SPOTS], flat[SPOTS:])
        convolve(moved, w1, accs)
        for spot in range(SPOTS):
            for n in range(2):
                got = jnp.maximum(pltpu.matmul_pop(accs[n][spot]), 0.0)
                hidden[spot, :, pl.ds(n * HALF, HALF)] = got.astype(jnp.bfloat16)
        convolve(hidden, w2, accs)
        for spot in range(SPOTS):
            for n in range(2):
                cols = pl.ds(n * HALF, HALF)
                got = jnp.maximum(pltpu.matmul_pop(accs[n][spot]), 0.0)
                got = got + moved[spot, :, cols].astype(jnp.float32)
                if spot:
                    got = jnp.maximum(got, pooled[:, cols])
                pooled[:, cols] = got

    pl.run_scoped(
        both,
        *[pltpu.ACC(n)((targets, HALF), jnp.float32) for n in range(2) for _ in range(SPOTS)],
    )

    core, y = lax.axis_index("core"), lax.axis_index("y")
    firsts = []
    for steps, swap in columns:
        first = lax.rem(y + steps, lax.axis_size("y")) * (2 * deep)
        firsts.append(first + (1 - core if swap else core))
    wide = (targets, 128)
    lane = lax.broadcasted_iota(jnp.int32, wide, 1)
    line = lax.broadcasted_iota(jnp.int32, wide, 0)
    place = 2 * (line & (deep - 1))
    for i, first in enumerate(firsts):
        place = place + jnp.where(line // deep == i, first, 0)
    few = labels.shape[1]
    spread_labels = jnp.broadcast_to(labels[...].astype(jnp.float32), (targets, few))
    mine = jnp.where(place[:, :few] == lane[:, :few], spread_labels, 0.0)
    label = jnp.sum(mine, axis=1, keepdims=True).astype(jnp.int32)
    logits = jnp.full(wide, -1e30, jnp.float32)
    for k in range(CLASSES):
        total = pooled[:, pl.ds(0, 128)] * head[k, :, pl.ds(0, 128)]
        for j in range(1, 4):
            cols = pl.ds(j * 128, 128)
            total = total + pooled[:, cols] * head[k, :, cols]
        logits = jnp.where(lane == k, jnp.sum(total, axis=1, keepdims=True), logits)
    chosen = lane == label
    correct = jnp.sum(jnp.where(chosen, logits, 0.0), axis=1, keepdims=True)
    rival = jnp.max(jnp.where(chosen, -1e30, logits), axis=1, keepdims=True)
    packed = jnp.where(lane < 64, correct - rival, ident[0].astype(jnp.float32))
    for i in range(targets):
        out[pl.ds(firsts[i // deep] + 2 * (i % deep), 1), 0, :] = packed[i : i + 1, :]


def in_vmem(x):
    return pltpu.with_memory_space_constraint(x, pltpu.VMEM)


def conv_call(columns, grids, ident, labels, head, w1, w2, before=None):
    targets = sum(grid.shape[0] for grid in grids)
    operands = [ident, labels, head, *map(in_vmem, (w1, w2, *grids))]
    aliases = {}
    if before is not None:
        aliases = {len(operands): 0}
        operands.append(in_vmem(before))
    vmem = pl.BlockSpec(memory_space=pltpu.VMEM)
    work = 2 * 100 * targets * 512 * 512 * 2
    return pl.pallas_call(
        functools.partial(conv_kernel, columns),
        out_shape=pltpu.VMEM((64, 1, 128), jnp.float32),
        in_specs=[pl.BlockSpec(memory_space=pltpu.SMEM)] + [vmem] * (len(operands) - 1),
        out_specs=vmem,
        scratch_shapes=[
            pltpu.VMEM((SPOTS, targets, 512), jnp.bfloat16),
            pltpu.VMEM((SPOTS, targets, 512), jnp.bfloat16),
            pltpu.VMEM((targets, 512), jnp.float32),
        ],
        input_output_aliases=aliases,
        cost_estimate=pl.CostEstimate(flops=work, bytes_accessed=1 << 20, transcendentals=0),
        compiler_params=pltpu.CompilerParams(vmem_limit_bytes=16 * 1024 * 1024),
        name=f"margins_{columns[0][0]}_{int(columns[0][1])}",
    )(*operands)


def spread_kernel(grid, out):
    flat = grid[...].reshape(SPOTS, grid.shape[-1])
    for i in range(out.shape[0]):
        out[i] = flat


def spread_call(grid, copies):
    return pl.pallas_call(
        spread_kernel,
        out_shape=pltpu.VMEM((copies, SPOTS, grid.shape[-1]), grid.dtype),
        in_specs=[pl.BlockSpec(memory_space=pltpu.VMEM)],
        out_specs=pl.BlockSpec(memory_space=pltpu.VMEM),
        cost_estimate=pl.CostEstimate(flops=10**10, bytes_accessed=1 << 25, transcendentals=0),
        compiler_params=pltpu.CompilerParams(vmem_limit_bytes=1024 * 1024),
        name="spread",
    )(grid)


def tail_kernel(columns, datamodel, mean_out, norm_out):
    models = columns.shape[0]
    rows = columns[:, 0, :]
    lane = lax.broadcasted_iota(jnp.int32, rows.shape, 1)
    margin = jnp.max(jnp.where(lane < 64, rows, -3e38), axis=1, keepdims=True)
    ident = jnp.max(jnp.where(lane < 64, -1.0, rows), axis=1, keepdims=True)
    mean = jnp.sum(margin, axis=0, keepdims=True) / models
    centred = margin - mean
    norm = jnp.sqrt(1.0 + jnp.sum(centred * centred, axis=0, keepdims=True) / models)
    scaled = centred / norm
    subset = lax.broadcasted_iota(jnp.int32, (models, SUBSETS), 1).astype(jnp.float32)
    datamodel[...] = jnp.sum(jnp.where(subset == ident, scaled, 0.0), axis=0, keepdims=True)
    mean_out[...] = jnp.broadcast_to(mean, mean_out.shape)
    norm_out[...] = jnp.broadcast_to(norm, norm_out.shape)


def tail_call(columns):
    vmem = pl.BlockSpec(memory_space=pltpu.VMEM)
    return pl.pallas_call(
        tail_kernel,
        out_shape=(
            jax.ShapeDtypeStruct((1, SUBSETS), jnp.float32),
            jax.ShapeDtypeStruct((1, 128), jnp.float32),
            jax.ShapeDtypeStruct((1, 128), jnp.float32),
        ),
        in_specs=[vmem],
        out_specs=(vmem, vmem, vmem),
        compiler_params=pltpu.CompilerParams(vmem_limit_bytes=1024 * 1024),
        name="statistics",
    )(columns)


def exchanged(x, axis):
    return lax.all_to_all(x, axis, 0, 0, tiled=True)


def shifted(x, axis, step):
    size = lax.axis_size(axis)
    return lax.ppermute(x, axis, [(i, (i + step) % size) for i in range(size)])


def shards(features, labels, subset_ids, conv1_weight, conv2_weight, head_weight):
    column = exchanged(spread_call(features[0], lax.axis_size("z")), "z")
    head = jnp.transpose(head_weight, (2, 0, 1))
    fixed = (subset_ids, labels.reshape(1, -1), head, conv1_weight[0], conv2_weight[0])
    column_o = shifted(column, "core", 1)
    three, one = shifted(column, "y", 1), shifted(column, "y", -1)
    column, column_o = lax.optimization_barrier((column, column_o))
    two = shifted(column, "y", 2)
    packed = conv_call(((0, False), (0, True)), (column, column_o), *fixed)
    three, one, packed = lax.optimization_barrier((three, one, packed))
    three_o, one_o = shifted(three, "core", 1), shifted(one, "core", 1)
    packed = conv_call(((3, False), (1, False)), (three, one), *fixed, packed)
    two, packed = lax.optimization_barrier((two, packed))
    two_o = shifted(two, "core", 1)
    packed = conv_call(((3, True), (1, True)), (three_o, one_o), *fixed, packed)
    packed = conv_call(((2, False), (2, True)), (two, two_o), *fixed, packed)
    columns = exchanged(packed, ("y", "z", "core"))
    datamodel, mean, norm = tail_call(columns)
    return (datamodel, mean[0, :1], norm[0, :1])


def solution(mesh):
    fine = Mesh(mesh.devices.reshape(4, 8, 2, 4), ("y", "z", "core", "dp"))
    mp = ("y", "z", "core")
    every = ("dp", *mp)
    in_specs = (
        P(every, None, None, None),
        P("dp"),
        P(mp),
        P(mp, None, None, None),
        P(mp, None, None, None),
        P(mp, None, None),
    )
    out_specs = (P(every, None), P(every), P(every))
    return jax.shard_map(shards, mesh=fine, in_specs=in_specs, out_specs=out_specs, check_vma=False)
```

```python
import functools

import jax
import jax.numpy as jnp
from jax import lax
from jax.experimental import pallas as pl
from jax.experimental.pallas import tpu as pltpu
from jax.sharding import Mesh, PartitionSpec as P


SIDE = 4
SPOTS = SIDE * SIDE
HALF = 256
CLASSES = 10
SUBSETS = 256
GROUP = 16

OFFSETS = (0, 1, 2, 3, 5, 6, 7, 8, 4)


def pairs_of(offset):
    row_off, col_off = offset // 3 - 1, offset % 3 - 1
    return [
        (r * SIDE + c, (r + row_off) * SIDE + c + col_off)
        for r in range(SIDE)
        for c in range(SIDE)
        if 0 <= r + row_off < SIDE and 0 <= c + col_off < SIDE
    ]


def convolve(source, weight, accs):
    stage = 0
    for offset in OFFSETS:
        pairs = pairs_of(offset)
        for k in range(2):
            deep = pl.ds(k * HALF, HALF)
            for n in range(2):
                pltpu.matmul_push_rhs(
                    weight[offset, deep, pl.ds(n * HALF, HALF)], staging_register=stage, mxu_index=n
                )
            for i, (spot, origin) in enumerate(pairs):
                rows = source[origin, :, deep]
                for n in range(2):
                    pltpu.matmul_acc_lhs(
                        accs[n][spot], rows, load_staged_rhs=stage if i == 0 else None
                    )
            stage = 1 - stage


def by_position(sources, moved, accs):
    lane = lax.broadcasted_iota(jnp.int32, (GROUP, HALF), 1)
    target = lax.broadcasted_iota(jnp.int32, (GROUP, HALF), 0)
    picks = [
        jnp.where(lane == target * SPOTS + spot, 1.0, 0.0).astype(jnp.bfloat16)
        for spot in range(SPOTS)
    ]
    pick = jnp.concatenate(picks, axis=0)
    for g, refs in enumerate(sources):
        for n in range(2):
            block = [ref[:, :, pl.ds(n * HALF, HALF)].reshape(-1, HALF) for ref in refs]
            pltpu.matmul_push_rhs(
                jnp.concatenate(block, axis=0), staging_register=g % 2, mxu_index=n
            )
            pltpu.matmul_acc_lhs(accs[n][g], pick, load_staged_rhs=g % 2)
    for g in range(len(sources)):
        for n in range(2):
            got = pltpu.matmul_pop(accs[n][g]).astype(jnp.bfloat16)
            moved[:, pl.ds(g * GROUP, GROUP), pl.ds(n * HALF, HALF)] = got.reshape(SPOTS, GROUP, HALF)


def conv_kernel(columns, *refs):
    labels, head, w1, w2 = refs[:4]
    grids = refs[4 : 4 + len(columns)]
    ident = refs[5 + len(columns)] if len(refs) == 10 + len(columns) else None
    out, moved, hidden, pooled = refs[-4:]
    targets = moved.shape[1]
    deep = grids[0].shape[0]
    groups = targets // GROUP
    sources = [grids[2 * g : 2 * g + 2] for g in range(groups)]

    def shuffle(*flat):
        by_position(sources, moved, (flat[:groups], flat[groups:]))

    pl.run_scoped(
        shuffle,
        *[pltpu.ACC(n)((HALF, HALF), jnp.float32) for n in range(2) for _ in range(groups)],
    )

    def both(*flat):
        accs = (flat[:SPOTS], flat[SPOTS:])
        convolve(moved, w1, accs)
        for spot in range(SPOTS):
            for n in range(2):
                got = jnp.maximum(pltpu.matmul_pop(accs[n][spot]), 0.0)
                hidden[spot, :, pl.ds(n * HALF, HALF)] = got.astype(jnp.bfloat16)
        convolve(hidden, w2, accs)
        for spot in range(SPOTS):
            for n in range(2):
                cols = pl.ds(n * HALF, HALF)
                got = jnp.maximum(pltpu.matmul_pop(accs[n][spot]), 0.0)
                got = got + moved[spot, :, cols].astype(jnp.float32)
                if spot:
                    got = jnp.maximum(got, pooled[:, cols])
                pooled[:, cols] = got

    pl.run_scoped(
        both,
        *[pltpu.ACC(n)((targets, HALF), jnp.float32) for n in range(2) for _ in range(SPOTS)],
    )

    core, y = lax.axis_index("core"), lax.axis_index("y")
    firsts = []
    for mask, swap in columns:
        first = lax.bitwise_xor(y, jnp.int32(mask)) * (2 * deep)
        firsts.append(first + (1 - core if swap else core))
    wide = (targets, 128)
    lane = lax.broadcasted_iota(jnp.int32, wide, 1)
    line = lax.broadcasted_iota(jnp.int32, wide, 0)
    place = 2 * (line & (deep - 1))
    for i, first in enumerate(firsts):
        place = place + jnp.where(line // deep == i, first, 0)
    few = labels.shape[1]
    spread_labels = jnp.broadcast_to(labels[...].astype(jnp.float32), (targets, few))
    mine = jnp.where(place[:, :few] == lane[:, :few], spread_labels, 0.0)
    label = jnp.sum(mine, axis=1, keepdims=True).astype(jnp.int32)
    logits = jnp.full(wide, -1e30, jnp.float32)
    for k in range(CLASSES):
        total = pooled[:, pl.ds(0, 128)] * head[k, :, pl.ds(0, 128)]
        for j in range(1, 4):
            cols = pl.ds(j * 128, 128)
            total = total + pooled[:, cols] * head[k, :, cols]
        logits = jnp.where(lane == k, jnp.sum(total, axis=1, keepdims=True), logits)
    chosen = lane == label
    correct = jnp.sum(jnp.where(chosen, logits, 0.0), axis=1, keepdims=True)
    rival = jnp.max(jnp.where(chosen, -1e30, logits), axis=1, keepdims=True)
    packed = jnp.broadcast_to(correct - rival, wide)
    for i in range(targets):
        out[pl.ds(firsts[i // deep] + 2 * (i % deep), 1), 0, :] = packed[i : i + 1, :]
    if ident is not None:
        whole = out[...]
        low = lax.broadcasted_iota(jnp.int32, whole.shape, 2) < 64
        out[...] = jnp.where(low, whole, ident[0].astype(jnp.float32))


def in_vmem(x):
    return pltpu.with_memory_space_constraint(x, pltpu.VMEM)


def conv_call(columns, grids, labels, head, w1, w2, before=None, ident=None):
    targets = sum(grid.shape[0] for grid in grids)
    vmem = pl.BlockSpec(memory_space=pltpu.VMEM)
    operands = [labels, head, *map(in_vmem, (w1, w2, *grids))]
    specs = [vmem] * len(operands)
    aliases = {}
    if before is not None:
        aliases = {len(operands): 0}
        operands.append(in_vmem(before))
        specs.append(vmem)
    if ident is not None:
        operands.append(ident)
        specs.append(pl.BlockSpec(memory_space=pltpu.SMEM))
    work = 2 * 100 * targets * 512 * 512 * 2
    return pl.pallas_call(
        functools.partial(conv_kernel, columns),
        out_shape=pltpu.VMEM((64, 1, 128), jnp.float32),
        in_specs=specs,
        out_specs=vmem,
        scratch_shapes=[
            pltpu.VMEM((SPOTS, targets, 512), jnp.bfloat16),
            pltpu.VMEM((SPOTS, targets, 512), jnp.bfloat16),
            pltpu.VMEM((targets, 512), jnp.float32),
        ],
        input_output_aliases=aliases,
        cost_estimate=pl.CostEstimate(flops=work, bytes_accessed=1 << 20, transcendentals=0),
        compiler_params=pltpu.CompilerParams(vmem_limit_bytes=16 * 1024 * 1024),
    )(*operands)


def spread_kernel(grid, out):
    flat = grid[...].reshape(SPOTS, grid.shape[-1])
    for i in range(out.shape[0]):
        out[i] = flat


def spread_call(grid, copies):
    return pl.pallas_call(
        spread_kernel,
        out_shape=pltpu.VMEM((copies, SPOTS, grid.shape[-1]), grid.dtype),
        in_specs=[pl.BlockSpec(memory_space=pltpu.VMEM)],
        out_specs=pl.BlockSpec(memory_space=pltpu.VMEM),
        cost_estimate=pl.CostEstimate(flops=10**10, bytes_accessed=1 << 25, transcendentals=0),
        compiler_params=pltpu.CompilerParams(vmem_limit_bytes=1024 * 1024),
        name="spread",
    )(grid)


def tail_kernel(columns, datamodel, mean_out, norm_out):
    models = columns.shape[0]
    rows = columns[:, 0, :]
    lane = lax.broadcasted_iota(jnp.int32, rows.shape, 1)
    margin = jnp.max(jnp.where(lane < 64, rows, -3e38), axis=1, keepdims=True)
    ident = jnp.max(jnp.where(lane < 64, -1.0, rows), axis=1, keepdims=True)
    mean = jnp.sum(margin, axis=0, keepdims=True) / models
    centred = margin - mean
    norm = jnp.sqrt(1.0 + jnp.sum(centred * centred, axis=0, keepdims=True) / models)
    scaled = centred / norm
    subset = lax.broadcasted_iota(jnp.int32, (models, SUBSETS), 1).astype(jnp.float32)
    datamodel[...] = jnp.sum(jnp.where(subset == ident, scaled, 0.0), axis=0, keepdims=True)
    mean_out[...] = jnp.broadcast_to(mean, mean_out.shape)
    norm_out[...] = jnp.broadcast_to(norm, norm_out.shape)


def tail_call(columns):
    vmem = pl.BlockSpec(memory_space=pltpu.VMEM)
    return pl.pallas_call(
        tail_kernel,
        out_shape=(
            jax.ShapeDtypeStruct((1, SUBSETS), jnp.float32),
            jax.ShapeDtypeStruct((1, 128), jnp.float32),
            jax.ShapeDtypeStruct((1, 128), jnp.float32),
        ),
        in_specs=[vmem],
        out_specs=(vmem, vmem, vmem),
        compiler_params=pltpu.CompilerParams(vmem_limit_bytes=1024 * 1024),
        name="statistics",
    )(columns)


def exchanged(x, axis):
    return lax.all_to_all(x, axis, 0, 0, tiled=True)


def swapped(x, axis, mask):
    return lax.ppermute(x, axis, [(i, i ^ mask) for i in range(lax.axis_size(axis))])


def staged(features, labels, subset_ids, conv1_weight, conv2_weight, head_weight):
    column = exchanged(spread_call(features[0], lax.axis_size("z")), "z")
    head = jnp.transpose(head_weight, (2, 0, 1))
    fixed = (labels.reshape(1, -1), head, conv1_weight[0], conv2_weight[0])
    column_o = swapped(column, "core", 1)
    near = swapped(column, "y", 3)
    next_ = swapped(column, "y", 1)
    far = swapped(column, "y", 2)
    packed = conv_call(((0, False), (0, True)), (column, column_o), *fixed)
    near, next_, packed = lax.optimization_barrier((near, next_, packed))
    near_o, next_o = swapped(near, "core", 1), swapped(next_, "core", 1)
    packed = conv_call(((3, False), (1, False)), (near, next_), *fixed, packed)
    far, packed = lax.optimization_barrier((far, packed))
    far_o = swapped(far, "core", 1)
    packed = conv_call(((3, True), (1, True)), (near_o, next_o), *fixed, packed)
    ident, packed = lax.optimization_barrier((subset_ids, packed))
    packed = conv_call(((2, False), (2, True)), (far, far_o), *fixed, packed, ident)
    columns = exchanged(packed, ("y", "z", "core"))
    datamodel, mean, norm = tail_call(columns)
    return (datamodel, mean[0, :1], norm[0, :1])


def solution(mesh):
    fine = Mesh(mesh.devices.reshape(4, 8, 2, 4), ("y", "z", "core", "dp"))
    mp = ("y", "z", "core")
    every = ("dp", *mp)
    in_specs = (
        P(every, None, None, None),
        P("dp"),
        P(mp),
        P(mp, None, None, None),
        P(mp, None, None, None),
        P(mp, None, None),
    )
    out_specs = (P(every, None), P(every), P(every))
    return jax.shard_map(staged, mesh=fine, in_specs=in_specs, out_specs=out_specs, check_vma=False)
```

```python
import functools

import jax
import jax.numpy as jnp
from jax import lax
from jax.experimental import pallas as pl
from jax.experimental.pallas import tpu as pltpu
from jax.sharding import Mesh, PartitionSpec as P


SIDE = 4
SPOTS = SIDE * SIDE
HALF = 256
CLASSES = 10
SUBSETS = 256
GROUP = 16

OFFSETS = (0, 1, 2, 3, 5, 6, 7, 8, 4)


def pairs_of(offset):
    row_off, col_off = offset // 3 - 1, offset % 3 - 1
    return [
        (r * SIDE + c, (r + row_off) * SIDE + c + col_off)
        for r in range(SIDE)
        for c in range(SIDE)
        if 0 <= r + row_off < SIDE and 0 <= c + col_off < SIDE
    ]


def convolve(source, weight, accs):
    stage = 0
    for offset in OFFSETS:
        pairs = pairs_of(offset)
        for k in range(2):
            deep = pl.ds(k * HALF, HALF)
            for n in range(2):
                pltpu.matmul_push_rhs(
                    weight[offset, deep, pl.ds(n * HALF, HALF)], staging_register=stage, mxu_index=n
                )
            for i, (spot, origin) in enumerate(pairs):
                rows = source[origin, :, deep]
                for n in range(2):
                    pltpu.matmul_acc_lhs(
                        accs[n][spot], rows, load_staged_rhs=stage if i == 0 else None
                    )
            stage = 1 - stage


def by_position(sources, moved, accs):
    lane = lax.broadcasted_iota(jnp.int32, (GROUP, HALF), 1)
    target = lax.broadcasted_iota(jnp.int32, (GROUP, HALF), 0)
    picks = [
        jnp.where(lane == target * SPOTS + spot, 1.0, 0.0).astype(jnp.bfloat16)
        for spot in range(SPOTS)
    ]
    pick = jnp.concatenate(picks, axis=0)
    for g, refs in enumerate(sources):
        for n in range(2):
            block = [ref[:, :, pl.ds(n * HALF, HALF)].reshape(-1, HALF) for ref in refs]
            pltpu.matmul_push_rhs(
                jnp.concatenate(block, axis=0), staging_register=g % 2, mxu_index=n
            )
            pltpu.matmul_acc_lhs(accs[n][g], pick, load_staged_rhs=g % 2)
    for g in range(len(sources)):
        for n in range(2):
            got = pltpu.matmul_pop(accs[n][g]).astype(jnp.bfloat16)
            moved[:, pl.ds(g * GROUP, GROUP), pl.ds(n * HALF, HALF)] = got.reshape(SPOTS, GROUP, HALF)


def margins_of(pooled, label, head):
    wide = (pooled.shape[0], 128)
    lane = lax.broadcasted_iota(jnp.int32, wide, 1)
    logits = jnp.full(wide, -1e30, jnp.float32)
    for k in range(CLASSES):
        total = pooled[:, :128] * head[k, :, pl.ds(0, 128)]
        for j in range(1, 4):
            total = total + pooled[:, j * 128 : j * 128 + 128] * head[k, :, pl.ds(j * 128, 128)]
        logits = jnp.where(lane == k, jnp.sum(total, axis=1, keepdims=True), logits)
    chosen = lane == label
    correct = jnp.sum(jnp.where(chosen, logits, 0.0), axis=1, keepdims=True)
    rival = jnp.max(jnp.where(chosen, -1e30, logits), axis=1, keepdims=True)
    return correct - rival


def conv_kernel(columns, step, last, *refs):
    refs = list(refs)
    w1, w2, *grids = refs[: 2 + len(columns[step])]
    refs = refs[2 + len(columns[step]) :]
    if step:
        before = refs.pop(0)
    if last:
        labels, head, ident, out = refs[:4]
    else:
        store = refs[0]
    moved, hidden = refs[-2:]
    targets = moved.shape[1]
    deep = grids[0].shape[0]
    groups = targets // GROUP
    sources = [grids[2 * g : 2 * g + 2] for g in range(groups)]

    if last:
        core, y = lax.axis_index("core"), lax.axis_index("y")
        wide = (targets, 128)
        lane = lax.broadcasted_iota(jnp.int32, wide, 1)
        line = lax.broadcasted_iota(jnp.int32, wide, 0)
        few = labels.shape[1]
        spread_labels = jnp.broadcast_to(labels[...].astype(jnp.float32), (targets, few))

        def send(part, pooled):
            firsts = []
            for mask, swap in columns[part]:
                first = lax.bitwise_xor(y, jnp.int32(mask)) * (2 * deep)
                firsts.append(first + (1 - core if swap else core))
            place = 2 * (line & (deep - 1))
            for i, first in enumerate(firsts):
                place = place + jnp.where(line // deep == i, first, 0)
            mine = jnp.where(place[:, :few] == lane[:, :few], spread_labels, 0.0)
            label = jnp.sum(mine, axis=1, keepdims=True).astype(jnp.int32)
            margin = margins_of(pooled, label, head)
            packed = jnp.where(lane < 64, margin, ident[0].astype(jnp.float32))
            for i in range(targets):
                out[pl.ds(firsts[i // deep] + 2 * (i % deep), 1), 0, :] = packed[i : i + 1, :]

    def shuffle(*flat):
        by_position(sources, moved, (flat[:groups], flat[groups:]))

    pl.run_scoped(
        shuffle,
        *[pltpu.ACC(n)((HALF, HALF), jnp.float32) for n in range(2) for _ in range(groups)],
    )
    if last:
        for part in range(step):
            send(part, before[pl.ds(part * targets, targets), :])

    def both(*flat):
        accs = (flat[:SPOTS], flat[SPOTS:])
        convolve(moved, w1, accs)
        for spot in range(SPOTS):
            for n in range(2):
                got = jnp.maximum(pltpu.matmul_pop(accs[n][spot]), 0.0)
                hidden[spot, :, pl.ds(n * HALF, HALF)] = got.astype(jnp.bfloat16)
        convolve(hidden, w2, accs)
        best = [None, None]
        for spot in range(SPOTS):
            for n in range(2):
                got = jnp.maximum(pltpu.matmul_pop(accs[n][spot]), 0.0)
                got = got + moved[spot, :, pl.ds(n * HALF, HALF)].astype(jnp.float32)
                best[n] = jnp.maximum(best[n], got) if spot else got
        pooled = jnp.concatenate(best, axis=1)
        if last:
            send(step, pooled)
        else:
            store[pl.ds(step * targets, targets), :] = pooled

    pl.run_scoped(
        both,
        *[pltpu.ACC(n)((targets, HALF), jnp.float32) for n in range(2) for _ in range(SPOTS)],
    )


def in_vmem(x):
    return pltpu.with_memory_space_constraint(x, pltpu.VMEM)


def conv_call(columns, step, grids, w1, w2, before=None, tail=None):
    targets = sum(grid.shape[0] for grid in grids)
    vmem = pl.BlockSpec(memory_space=pltpu.VMEM)
    operands = [*map(in_vmem, (w1, w2, *grids))]
    aliases = {}
    if before is not None:
        if tail is None:
            aliases = {len(operands): 0}
        operands.append(in_vmem(before))
    specs = [vmem] * len(operands)
    if tail is None:
        out_shape = pltpu.VMEM((targets * len(columns), 512), jnp.float32)
    else:
        operands += tail
        specs += [vmem, vmem, pl.BlockSpec(memory_space=pltpu.SMEM)]
        out_shape = pltpu.VMEM((targets * len(columns), 1, 128), jnp.float32)
    work = 2 * 100 * targets * 512 * 512 * 2
    return pl.pallas_call(
        functools.partial(conv_kernel, columns, step, tail is not None),
        out_shape=out_shape,
        in_specs=specs,
        out_specs=vmem,
        scratch_shapes=[
            pltpu.VMEM((SPOTS, targets, 512), jnp.bfloat16),
            pltpu.VMEM((SPOTS, targets, 512), jnp.bfloat16),
        ],
        input_output_aliases=aliases,
        cost_estimate=pl.CostEstimate(flops=work, bytes_accessed=1 << 20, transcendentals=0),
        compiler_params=pltpu.CompilerParams(vmem_limit_bytes=16 * 1024 * 1024),
    )(*operands)


def spread_kernel(grid, out):
    flat = grid[...].reshape(SPOTS, grid.shape[-1])
    for i in range(out.shape[0]):
        out[i] = flat


def spread_call(grid, copies):
    return pl.pallas_call(
        spread_kernel,
        out_shape=pltpu.VMEM((copies, SPOTS, grid.shape[-1]), grid.dtype),
        in_specs=[pl.BlockSpec(memory_space=pltpu.VMEM)],
        out_specs=pl.BlockSpec(memory_space=pltpu.VMEM),
        cost_estimate=pl.CostEstimate(flops=10**10, bytes_accessed=1 << 25, transcendentals=0),
        compiler_params=pltpu.CompilerParams(vmem_limit_bytes=1024 * 1024),
        name="spread",
    )(grid)


def tail_kernel(columns, datamodel, mean_out, norm_out):
    models = columns.shape[0]
    rows = columns[:, 0, :]
    lane = lax.broadcasted_iota(jnp.int32, rows.shape, 1)
    margin = jnp.max(jnp.where(lane < 64, rows, -3e38), axis=1, keepdims=True)
    ident = jnp.max(jnp.where(lane < 64, -1.0, rows), axis=1, keepdims=True)
    mean = jnp.sum(margin, axis=0, keepdims=True) / models
    centred = margin - mean
    norm = jnp.sqrt(1.0 + jnp.sum(centred * centred, axis=0, keepdims=True) / models)
    scaled = centred / norm
    subset = lax.broadcasted_iota(jnp.int32, (models, SUBSETS), 1).astype(jnp.float32)
    datamodel[...] = jnp.sum(jnp.where(subset == ident, scaled, 0.0), axis=0, keepdims=True)
    mean_out[...] = jnp.broadcast_to(mean, mean_out.shape)
    norm_out[...] = jnp.broadcast_to(norm, norm_out.shape)


def tail_call(columns):
    vmem = pl.BlockSpec(memory_space=pltpu.VMEM)
    return pl.pallas_call(
        tail_kernel,
        out_shape=(
            jax.ShapeDtypeStruct((1, SUBSETS), jnp.float32),
            jax.ShapeDtypeStruct((1, 128), jnp.float32),
            jax.ShapeDtypeStruct((1, 128), jnp.float32),
        ),
        in_specs=[vmem],
        out_specs=(vmem, vmem, vmem),
        compiler_params=pltpu.CompilerParams(vmem_limit_bytes=1024 * 1024),
        name="statistics",
    )(columns)


def exchanged(x, axis):
    return lax.all_to_all(x, axis, 0, 0, tiled=True)


def swapped(x, axis, mask):
    return lax.ppermute(x, axis, [(i, i ^ mask) for i in range(lax.axis_size(axis))])


def staged(features, labels, subset_ids, conv1_weight, conv2_weight, head_weight):
    column = exchanged(spread_call(features[0], lax.axis_size("z")), "z")
    head = jnp.transpose(head_weight, (2, 0, 1))
    fixed = (conv1_weight[0], conv2_weight[0])
    column_o = swapped(column, "core", 1)
    near = swapped(column, "y", 1)
    next_ = swapped(column, "y", 3)
    far = swapped(column, "y", 2)
    plan = (
        ((0, False), (0, True)),
        ((1, False), (3, False)),
        ((1, True), (3, True)),
        ((2, False), (2, True)),
    )
    pooled = conv_call(plan, 0, (column, column_o), *fixed)
    near, next_, pooled = lax.optimization_barrier((near, next_, pooled))
    near_o, next_o = swapped(near, "core", 1), swapped(next_, "core", 1)
    pooled = conv_call(plan, 1, (near, next_), *fixed, pooled)
    far, pooled = lax.optimization_barrier((far, pooled))
    far_o = swapped(far, "core", 1)
    pooled = conv_call(plan, 2, (near_o, next_o), *fixed, pooled)
    tail = (labels.reshape(1, -1), head, subset_ids)
    packed = conv_call(plan, 3, (far, far_o), *fixed, pooled, tail)
    columns = exchanged(packed, ("y", "z", "core"))
    datamodel, mean, norm = tail_call(columns)
    return (datamodel, mean[0, :1], norm[0, :1])


def solution(mesh):
    fine = Mesh(mesh.devices.reshape(4, 8, 2, 4), ("y", "z", "core", "dp"))
    mp = ("y", "z", "core")
    every = ("dp", *mp)
    in_specs = (
        P(every, None, None, None),
        P("dp"),
        P(mp),
        P(mp, None, None, None),
        P(mp, None, None, None),
        P(mp, None, None),
    )
    out_specs = (P(every, None), P(every), P(every))
    return jax.shard_map(staged, mesh=fine, in_specs=in_specs, out_specs=out_specs, check_vma=False)
```

```python
import functools

import jax
import jax.numpy as jnp
from jax import lax
from jax.experimental import pallas as pl
from jax.experimental.pallas import tpu as pltpu
from jax.sharding import Mesh, PartitionSpec as P


SIDE = 4
SPOTS = SIDE * SIDE
HALF = 256
CLASSES = 10
SUBSETS = 256
GROUP = 16

OFFSETS = (0, 1, 2, 3, 5, 6, 7, 8, 4)


def pairs_of(offset):
    row_off, col_off = offset // 3 - 1, offset % 3 - 1
    return [
        (r * SIDE + c, (r + row_off) * SIDE + c + col_off)
        for r in range(SIDE)
        for c in range(SIDE)
        if 0 <= r + row_off < SIDE and 0 <= c + col_off < SIDE
    ]


def convolve(source, weight, accs):
    stage = 0
    for offset in OFFSETS:
        pairs = pairs_of(offset)
        for k in range(2):
            deep = pl.ds(k * HALF, HALF)
            for n in range(2):
                pltpu.matmul_push_rhs(
                    weight[offset, deep, pl.ds(n * HALF, HALF)], staging_register=stage, mxu_index=n
                )
            for i, (spot, origin) in enumerate(pairs):
                rows = source[origin, :, deep]
                for n in range(2):
                    pltpu.matmul_acc_lhs(
                        accs[n][spot], rows, load_staged_rhs=stage if i == 0 else None
                    )
            stage = 1 - stage


def by_position(sources, moved, wide):
    for g, refs in enumerate(sources):
        at = 0
        for ref in refs:
            rows = ref.shape[0] * SPOTS
            for j in range(wide.shape[0]):
                part = ref[:, :, pl.ds(j * 128, 128)].reshape(rows, 128)
                wide[j, pl.ds(at, rows), :] = part.astype(jnp.float32)
            at += rows
        for spot in range(SPOTS):
            for j in range(wide.shape[0]):
                picked = wide[j, pl.ds(spot, GROUP, stride=SPOTS), :]
                moved[spot, pl.ds(g * GROUP, GROUP), pl.ds(j * 128, 128)] = picked.astype(jnp.bfloat16)


def margins_of(pooled, label, head):
    correct = jnp.zeros((pooled.shape[0], 1), jnp.float32)
    rival = jnp.full((pooled.shape[0], 1), -1e30, jnp.float32)
    for k in range(CLASSES):
        total = pooled[:, :128] * head[k, :, pl.ds(0, 128)]
        for j in range(1, 4):
            total = total + pooled[:, j * 128 : j * 128 + 128] * head[k, :, pl.ds(j * 128, 128)]
        logit = jnp.sum(total, axis=1, keepdims=True)
        correct = jnp.where(label == k, logit, correct)
        rival = jnp.where(label == k, rival, jnp.maximum(rival, logit))
    return correct - rival


def conv_kernel(columns, step, last, *refs):
    refs = list(refs)
    w1, w2, *grids = refs[: 2 + len(columns[step])]
    refs = refs[2 + len(columns[step]) :]
    if step:
        before = refs.pop(0)
    if last:
        labels, head, ident, out = refs[:4]
    else:
        store = refs[0]
    moved, hidden, wide = refs[-3:]
    targets = moved.shape[1]
    deep = grids[0].shape[0]
    groups = targets // GROUP
    sources = [grids[2 * g : 2 * g + 2] for g in range(groups)]

    if last:
        core, y = lax.axis_index("core"), lax.axis_index("y")
        lanes = (targets, 128)
        lane = lax.broadcasted_iota(jnp.int32, lanes, 1)
        line = lax.broadcasted_iota(jnp.int32, lanes, 0)
        few = labels.shape[1]
        spread_labels = jnp.broadcast_to(labels[...].astype(jnp.float32), (targets, few))

        def send(part, pooled):
            firsts = []
            for mask, swap in columns[part]:
                first = lax.bitwise_xor(y, jnp.int32(mask)) * (2 * deep)
                firsts.append(first + (1 - core if swap else core))
            place = 2 * (line & (deep - 1))
            for i, first in enumerate(firsts):
                place = place + jnp.where(line // deep == i, first, 0)
            mine = jnp.where(place[:, :few] == lane[:, :few], spread_labels, 0.0)
            label = jnp.sum(mine, axis=1, keepdims=True).astype(jnp.int32)
            margin = margins_of(pooled, label, head)
            packed = jnp.where(lane < 64, margin, ident[0].astype(jnp.float32))
            for i in range(targets):
                out[pl.ds(firsts[i // deep] + 2 * (i % deep), 1), 0, :] = packed[i : i + 1, :]

    by_position(sources, moved, wide)
    if last:
        for part in range(step):
            send(part, before[pl.ds(part * targets, targets), :])

    def both(*flat):
        accs = (flat[:SPOTS], flat[SPOTS:])
        convolve(moved, w1, accs)
        for spot in range(SPOTS):
            for n in range(2):
                got = jnp.maximum(pltpu.matmul_pop(accs[n][spot]), 0.0)
                hidden[spot, :, pl.ds(n * HALF, HALF)] = got.astype(jnp.bfloat16)
        convolve(hidden, w2, accs)
        best = [None, None]
        for spot in range(SPOTS):
            for n in range(2):
                got = jnp.maximum(pltpu.matmul_pop(accs[n][spot]), 0.0)
                got = got + moved[spot, :, pl.ds(n * HALF, HALF)].astype(jnp.float32)
                best[n] = jnp.maximum(best[n], got) if spot else got
        pooled = jnp.concatenate(best, axis=1)
        if last:
            send(step, pooled)
        else:
            store[pl.ds(step * targets, targets), :] = pooled

    pl.run_scoped(
        both,
        *[pltpu.ACC(n)((targets, HALF), jnp.float32) for n in range(2) for _ in range(SPOTS)],
    )


def in_vmem(x):
    return pltpu.with_memory_space_constraint(x, pltpu.VMEM)


def conv_call(columns, step, grids, w1, w2, before=None, tail=None):
    targets = sum(grid.shape[0] for grid in grids)
    vmem = pl.BlockSpec(memory_space=pltpu.VMEM)
    operands = [*map(in_vmem, (w1, w2, *grids))]
    aliases = {}
    if before is not None:
        if tail is None:
            aliases = {len(operands): 0}
        operands.append(in_vmem(before))
    specs = [vmem] * len(operands)
    if tail is None:
        out_shape = pltpu.VMEM((targets * len(columns), 512), jnp.float32)
    else:
        operands += tail
        specs += [vmem, vmem, pl.BlockSpec(memory_space=pltpu.SMEM)]
        out_shape = pltpu.VMEM((targets * len(columns), 1, 128), jnp.float32)
    work = 2 * 100 * targets * 512 * 512 * 2
    return pl.pallas_call(
        functools.partial(conv_kernel, columns, step, tail is not None),
        out_shape=out_shape,
        in_specs=specs,
        out_specs=vmem,
        scratch_shapes=[
            pltpu.VMEM((SPOTS, targets, 512), jnp.bfloat16),
            pltpu.VMEM((SPOTS, targets, 512), jnp.bfloat16),
            pltpu.VMEM((4, GROUP * SPOTS, 128), jnp.float32),
        ],
        input_output_aliases=aliases,
        cost_estimate=pl.CostEstimate(flops=work, bytes_accessed=1 << 20, transcendentals=0),
        compiler_params=pltpu.CompilerParams(vmem_limit_bytes=16 * 1024 * 1024),
    )(*operands)


def spread_kernel(grid, out):
    flat = grid[...].reshape(SPOTS, grid.shape[-1])
    for i in range(out.shape[0]):
        out[i] = flat


def spread_call(grid, copies):
    return pl.pallas_call(
        spread_kernel,
        out_shape=pltpu.VMEM((copies, SPOTS, grid.shape[-1]), grid.dtype),
        in_specs=[pl.BlockSpec(memory_space=pltpu.VMEM)],
        out_specs=pl.BlockSpec(memory_space=pltpu.VMEM),
        cost_estimate=pl.CostEstimate(flops=10**10, bytes_accessed=1 << 25, transcendentals=0),
        compiler_params=pltpu.CompilerParams(vmem_limit_bytes=1024 * 1024),
        name="spread",
    )(grid)


def tail_kernel(columns, datamodel, mean_out, norm_out):
    models = columns.shape[0]
    rows = columns[:, 0, :]
    turned = pltpu.roll(rows, 64, 1)
    lane = lax.broadcasted_iota(jnp.int32, rows.shape, 1)
    margin = jnp.where(lane < 64, rows, turned)
    ident = jnp.where(lane < 64, turned, rows)
    mean = jnp.sum(margin, axis=0, keepdims=True) / models
    centred = margin - mean
    norm = jnp.sqrt(1.0 + jnp.sum(centred * centred, axis=0, keepdims=True) / models)
    scaled = centred / norm
    for h in range(SUBSETS // 128):
        subset = (lane + 128 * h).astype(jnp.float32)
        datamodel[:, pl.ds(128 * h, 128)] = jnp.sum(
            jnp.where(subset == ident, scaled, 0.0), axis=0, keepdims=True
        )
    mean_out[...] = mean
    norm_out[...] = norm


def tail_call(columns):
    vmem = pl.BlockSpec(memory_space=pltpu.VMEM)
    return pl.pallas_call(
        tail_kernel,
        out_shape=(
            jax.ShapeDtypeStruct((1, SUBSETS), jnp.float32),
            jax.ShapeDtypeStruct((1, 128), jnp.float32),
            jax.ShapeDtypeStruct((1, 128), jnp.float32),
        ),
        in_specs=[vmem],
        out_specs=(vmem, vmem, vmem),
        compiler_params=pltpu.CompilerParams(vmem_limit_bytes=1024 * 1024),
        name="statistics",
    )(columns)


def exchanged(x, axis):
    return lax.all_to_all(x, axis, 0, 0, tiled=True)


def swapped(x, axis, mask):
    return lax.ppermute(x, axis, [(i, i ^ mask) for i in range(lax.axis_size(axis))])


def staged(features, labels, subset_ids, conv1_weight, conv2_weight, head_weight):
    column = exchanged(spread_call(features[0], lax.axis_size("z")), "z")
    head = jnp.transpose(head_weight, (2, 0, 1))
    fixed = (conv1_weight[0], conv2_weight[0])
    column_o = swapped(column, "core", 1)
    near = swapped(column, "y", 1)
    next_ = swapped(column, "y", 3)
    far = swapped(column, "y", 2)
    plan = (
        ((0, False), (0, True)),
        ((1, False), (3, False)),
        ((1, True), (3, True)),
        ((2, False), (2, True)),
    )
    pooled = conv_call(plan, 0, (column, column_o), *fixed)
    near, next_, pooled = lax.optimization_barrier((near, next_, pooled))
    near_o, next_o = swapped(near, "core", 1), swapped(next_, "core", 1)
    pooled = conv_call(plan, 1, (near, next_), *fixed, pooled)
    far, pooled = lax.optimization_barrier((far, pooled))
    far_o = swapped(far, "core", 1)
    pooled = conv_call(plan, 2, (near_o, next_o), *fixed, pooled)
    tail = (labels.reshape(1, -1), head, subset_ids)
    packed = conv_call(plan, 3, (far, far_o), *fixed, pooled, tail)
    columns = exchanged(packed, ("y", "z", "core"))
    datamodel, mean, norm = tail_call(columns)
    return (datamodel, mean[0, :1], norm[0, :1])


def solution(mesh):
    fine = Mesh(mesh.devices.reshape(4, 8, 2, 4), ("y", "z", "core", "dp"))
    mp = ("y", "z", "core")
    every = ("dp", *mp)
    in_specs = (
        P(every, None, None, None),
        P("dp"),
        P(mp),
        P(mp, None, None, None),
        P(mp, None, None, None),
        P(mp, None, None),
    )
    out_specs = (P(every, None), P(every), P(every))
    return jax.shard_map(staged, mesh=fine, in_specs=in_specs, out_specs=out_specs, check_vma=False)
```

```python
import functools

import jax
import jax.numpy as jnp
from jax import lax
from jax.experimental import pallas as pl
from jax.experimental.pallas import tpu as pltpu
from jax.sharding import Mesh, PartitionSpec as P


SIDE = 4
SPOTS = SIDE * SIDE
HALF = 256
CLASSES = 10
SUBSETS = 256
GROUP = 16

OFFSETS = (0, 1, 2, 3, 5, 6, 7, 8, 4)


def pairs_of(offset):
    row_off, col_off = offset // 3 - 1, offset % 3 - 1
    return [
        (r * SIDE + c, (r + row_off) * SIDE + c + col_off)
        for r in range(SIDE)
        for c in range(SIDE)
        if 0 <= r + row_off < SIDE and 0 <= c + col_off < SIDE
    ]


def convolve(source, weight, accs):
    stage = 0
    for offset in OFFSETS:
        pairs = pairs_of(offset)
        for k in range(2):
            deep = pl.ds(k * HALF, HALF)
            for n in range(2):
                pltpu.matmul_push_rhs(
                    weight[offset, deep, pl.ds(n * HALF, HALF)], staging_register=stage, mxu_index=n
                )
            for i, (spot, origin) in enumerate(pairs):
                rows = source[origin, :, deep]
                for n in range(2):
                    pltpu.matmul_acc_lhs(
                        accs[n][spot], rows, load_staged_rhs=stage if i == 0 else None
                    )
            stage = 1 - stage


def by_position(sources, moved, wide):
    for g, refs in enumerate(sources):
        at = 0
        for ref in refs:
            rows = ref.shape[0] * SPOTS
            for j in range(wide.shape[0]):
                part = ref[:, :, pl.ds(j * 128, 128)].reshape(rows, 128)
                wide[j, pl.ds(at, rows), :] = part.astype(jnp.float32)
            at += rows
        for spot in range(SPOTS):
            for j in range(wide.shape[0]):
                picked = wide[j, pl.ds(spot, GROUP, stride=SPOTS), :]
                moved[spot, pl.ds(g * GROUP, GROUP), pl.ds(j * 128, 128)] = picked.astype(jnp.bfloat16)


def margins_of(pooled, label, head):
    correct = jnp.zeros((pooled.shape[0], 1), jnp.float32)
    rival = jnp.full((pooled.shape[0], 1), -1e30, jnp.float32)
    for k in range(CLASSES):
        total = pooled[:, :128] * head[k, :, pl.ds(0, 128)]
        for j in range(1, 4):
            total = total + pooled[:, j * 128 : j * 128 + 128] * head[k, :, pl.ds(j * 128, 128)]
        logit = jnp.sum(total, axis=1, keepdims=True)
        correct = jnp.where(label == k, logit, correct)
        rival = jnp.where(label == k, rival, jnp.maximum(rival, logit))
    return correct - rival


def conv_kernel(columns, step, last, *refs):
    refs = list(refs)
    w1, w2, *grids = refs[: 2 + len(columns[step])]
    refs = refs[2 + len(columns[step]) :]
    if step:
        before = refs.pop(0)
    if last:
        labels, head, ident, out = refs[:4]
    else:
        store = refs[0]
    moved, hidden, wide = refs[-3:]
    targets = moved.shape[1]
    deep = grids[0].shape[0]
    groups = targets // GROUP
    sources = [grids[2 * g : 2 * g + 2] for g in range(groups)]

    if last:
        core, y = lax.axis_index("core"), lax.axis_index("y")
        lanes = (targets, 128)
        lane = lax.broadcasted_iota(jnp.int32, lanes, 1)
        line = lax.broadcasted_iota(jnp.int32, lanes, 0)
        few = labels.shape[1]
        spread_labels = jnp.broadcast_to(labels[...].astype(jnp.float32), (targets, few))

        def send(part, pooled):
            firsts = []
            for mask, swap in columns[part]:
                first = lax.bitwise_xor(y, jnp.int32(mask)) * (2 * deep)
                firsts.append(first + (1 - core if swap else core))
            place = 2 * (line & (deep - 1))
            for i, first in enumerate(firsts):
                place = place + jnp.where(line // deep == i, first, 0)
            mine = jnp.where(place[:, :few] == lane[:, :few], spread_labels, 0.0)
            label = jnp.sum(mine, axis=1, keepdims=True).astype(jnp.int32)
            margin = margins_of(pooled, label, head)
            packed = jnp.where(lane < 64, margin, ident[0].astype(jnp.float32))
            for i in range(targets):
                out[pl.ds(firsts[i // deep] + 2 * (i % deep), 1), 0, :] = packed[i : i + 1, :]

    by_position(sources, moved, wide)
    if last:
        for part in range(step):
            send(part, before[pl.ds(part * targets, targets), :])

    def both(*flat):
        accs = (flat[:SPOTS], flat[SPOTS:])
        convolve(moved, w1, accs)
        for spot in range(SPOTS):
            for n in range(2):
                got = jnp.maximum(pltpu.matmul_pop(accs[n][spot]), 0.0)
                hidden[spot, :, pl.ds(n * HALF, HALF)] = got.astype(jnp.bfloat16)
        convolve(hidden, w2, accs)
        best = [None, None]
        for spot in range(SPOTS):
            for n in range(2):
                got = jnp.maximum(pltpu.matmul_pop(accs[n][spot]), 0.0)
                got = got + moved[spot, :, pl.ds(n * HALF, HALF)].astype(jnp.float32)
                best[n] = jnp.maximum(best[n], got) if spot else got
        pooled = jnp.concatenate(best, axis=1)
        if last:
            send(step, pooled)
        else:
            store[pl.ds(step * targets, targets), :] = pooled

    pl.run_scoped(
        both,
        *[pltpu.ACC(n)((targets, HALF), jnp.float32) for n in range(2) for _ in range(SPOTS)],
    )


def in_vmem(x):
    return pltpu.with_memory_space_constraint(x, pltpu.VMEM)


def conv_call(columns, step, grids, w1, w2, before=None, tail=None):
    targets = sum(grid.shape[0] for grid in grids)
    vmem = pl.BlockSpec(memory_space=pltpu.VMEM)
    operands = [*map(in_vmem, (w1, w2, *grids))]
    aliases = {}
    if before is not None:
        if tail is None:
            aliases = {len(operands): 0}
        operands.append(in_vmem(before))
    specs = [vmem] * len(operands)
    if tail is None:
        out_shape = pltpu.VMEM((targets * len(columns), 512), jnp.float32)
    else:
        operands += tail
        specs += [vmem, vmem, pl.BlockSpec(memory_space=pltpu.SMEM)]
        out_shape = pltpu.VMEM((targets * len(columns), 1, 128), jnp.float32)
    work = 2 * 100 * targets * 512 * 512 * 2
    return pl.pallas_call(
        functools.partial(conv_kernel, columns, step, tail is not None),
        out_shape=out_shape,
        in_specs=specs,
        out_specs=vmem,
        scratch_shapes=[
            pltpu.VMEM((SPOTS, targets, 512), jnp.bfloat16),
            pltpu.VMEM((SPOTS, targets, 512), jnp.bfloat16),
            pltpu.VMEM((4, GROUP * SPOTS, 128), jnp.float32),
        ],
        input_output_aliases=aliases,
        cost_estimate=pl.CostEstimate(flops=work, bytes_accessed=1 << 20, transcendentals=0),
        compiler_params=pltpu.CompilerParams(vmem_limit_bytes=16 * 1024 * 1024),
    )(*operands)


def spread_kernel(grid, out):
    flat = grid[...].reshape(SPOTS, grid.shape[-1])
    for i in range(out.shape[0]):
        out[i] = flat


def spread_call(grid, copies):
    return pl.pallas_call(
        spread_kernel,
        out_shape=pltpu.VMEM((copies, SPOTS, grid.shape[-1]), grid.dtype),
        in_specs=[pl.BlockSpec(memory_space=pltpu.VMEM)],
        out_specs=pl.BlockSpec(memory_space=pltpu.VMEM),
        cost_estimate=pl.CostEstimate(flops=10**10, bytes_accessed=1 << 25, transcendentals=0),
        compiler_params=pltpu.CompilerParams(vmem_limit_bytes=1024 * 1024),
        name="spread",
    )(grid)


def tail_kernel(columns, datamodel, mean_out, norm_out):
    models = columns.shape[0]
    rows = columns[:, 0, :]
    turned = pltpu.roll(rows, 64, 1)
    lane = lax.broadcasted_iota(jnp.int32, rows.shape, 1)
    margin = jnp.where(lane < 64, rows, turned)
    ident = jnp.where(lane < 64, turned, rows)
    mean = jnp.sum(margin, axis=0, keepdims=True) / models
    centred = margin - mean
    norm = jnp.sqrt(1.0 + jnp.sum(centred * centred, axis=0, keepdims=True) / models)
    scaled = centred / norm
    for h in range(SUBSETS // 128):
        subset = (lane + 128 * h).astype(jnp.float32)
        datamodel[:, pl.ds(128 * h, 128)] = jnp.sum(
            jnp.where(subset == ident, scaled, 0.0), axis=0, keepdims=True
        )
    mean_out[...] = mean
    norm_out[...] = norm


def tail_call(columns):
    vmem = pl.BlockSpec(memory_space=pltpu.VMEM)
    return pl.pallas_call(
        tail_kernel,
        out_shape=(
            jax.ShapeDtypeStruct((1, SUBSETS), jnp.float32),
            jax.ShapeDtypeStruct((1, 128), jnp.float32),
            jax.ShapeDtypeStruct((1, 128), jnp.float32),
        ),
        in_specs=[vmem],
        out_specs=(vmem, vmem, vmem),
        compiler_params=pltpu.CompilerParams(vmem_limit_bytes=1024 * 1024),
        name="statistics",
    )(columns)


def exchanged(x, axis):
    return lax.all_to_all(x, axis, 0, 0, tiled=True)


def swapped(x, axis, mask):
    return lax.ppermute(x, axis, [(i, i ^ mask) for i in range(lax.axis_size(axis))])


def staged(features, labels, subset_ids, conv1_weight, conv2_weight, head_weight):
    column = exchanged(spread_call(features[0], lax.axis_size("z")), "z")
    head = jnp.transpose(head_weight, (2, 0, 1))
    fixed = (conv1_weight[0], conv2_weight[0])
    column_o = swapped(column, "core", 1)
    near = swapped(column, "y", 3)
    next_ = swapped(column, "y", 1)
    far = swapped(column, "y", 2)
    plan = (
        ((0, False), (0, True)),
        ((3, False), (1, False)),
        ((3, True), (1, True)),
        ((2, False), (2, True)),
    )
    pooled = conv_call(plan, 0, (column, column_o), *fixed)
    near, next_, pooled = lax.optimization_barrier((near, next_, pooled))
    near_o, next_o = swapped(near, "core", 1), swapped(next_, "core", 1)
    pooled = conv_call(plan, 1, (near, next_), *fixed, pooled)
    far, pooled = lax.optimization_barrier((far, pooled))
    far_o = swapped(far, "core", 1)
    pooled = conv_call(plan, 2, (near_o, next_o), *fixed, pooled)
    tail = (labels.reshape(1, -1), head, subset_ids)
    packed = conv_call(plan, 3, (far, far_o), *fixed, pooled, tail)
    columns = exchanged(packed, ("y", "z", "core"))
    datamodel, mean, norm = tail_call(columns)
    return (datamodel, mean[0, :1], norm[0, :1])


def solution(mesh):
    fine = Mesh(mesh.devices.reshape(4, 8, 2, 4), ("y", "z", "core", "dp"))
    mp = ("y", "z", "core")
    every = ("dp", *mp)
    in_specs = (
        P(every, None, None, None),
        P("dp"),
        P(mp),
        P(mp, None, None, None),
        P(mp, None, None, None),
        P(mp, None, None),
    )
    out_specs = (P(every, None), P(every), P(every))
    return jax.shard_map(staged, mesh=fine, in_specs=in_specs, out_specs=out_specs, check_vma=False)
```
